64 devices in a mesh: sys: 4 (over x, y), row: 16 (over z, core).
Axes of the slice: x: 2, y: 2, z: 8, core: 2. Of those that a mesh axis runs over, the one named last changes fastest.
The devices are a block of a 4x4x8 slice.
Arguments:
- positions: bfloat16 [131072, 128], P(('sys', 'row')), parts along dimension 0
- charges: float32 [131072], P(('sys', 'row')), parts along dimension 0
Outputs:
- output 1: float32 [131072, 128], P(('sys', 'row')), parts along dimension 0
- output 2: float32 [4], P('sys'), parts along dimension 0
There are 4 independent parts. The reference program is written for one: setup_inputs(seed, part) draws one part's arguments, and reference() takes and returns one part's arrays. A program takes and returns all parts, laid end to end along the dimension named above; each array names one.
All inputs are finite; a program needn't handle non-finite values.
Results may differ from the reference program's by a relative error of at most 0.001.
Values are sent between devices in bfloat16 or wider.
A program may use at most 768 MiB of HBM per device.

```python
import jax
import jax.numpy as jnp
from jax import lax

D = 128
ROWS_DEV = 2048
RING = 16
N_ROWS = ROWS_DEV * RING
ELL_SQ = float(D)


def setup_inputs(seed: int = 0, part: int = 0) -> dict:
    root_key = jax.random.key(seed)
    part_key = jax.random.fold_in(root_key, part)
    key_x, key_q = jax.random.split(part_key)
    positions = jax.random.normal(key_x, (N_ROWS, D), jnp.float32).astype(jnp.bfloat16)
    charges = jax.random.normal(key_q, (N_ROWS,), jnp.float32) * (N_ROWS ** -0.25)
    return {"positions": positions, "charges": charges}


def reference(positions, charges):
    sq_norm = jnp.sum(jnp.square(positions.astype(jnp.float32)), axis=1)
    blocks_x = positions.reshape(RING, ROWS_DEV, D)
    blocks_q = charges.reshape(RING, ROWS_DEV)
    blocks_sq = sq_norm.reshape(RING, ROWS_DEV)
    block_ids = jnp.arange(RING)
    local_ids = jnp.arange(ROWS_DEV)

    def row_block(host_in):
        host_x, host_q, host_sq, host_id = host_in

        def col_step(acc_state, col_in):
            force_acc, energy_acc = acc_state
            col_x, col_q, col_sq, col_id = col_in
            cross_dot = jnp.dot(host_x, col_x.T, preferred_element_type=jnp.float32)
            sq_dist = jnp.maximum(host_sq[:, None] + col_sq[None, :] - 2.0 * cross_dot, 0.0)
            is_self = (host_id * ROWS_DEV + local_ids)[:, None] == (col_id * ROWS_DEV + local_ids)[None, :]
            weight = jnp.where(is_self, 0.0, host_q[:, None] * col_q[None, :] * jnp.exp(-sq_dist / (2.0 * ELL_SQ)))
            pulled = jnp.dot(weight.astype(jnp.bfloat16), col_x, preferred_element_type=jnp.float32)
            force_acc = force_acc + jnp.sum(weight, axis=1)[:, None] * host_x.astype(jnp.float32) - pulled
            return (force_acc, energy_acc + jnp.sum(weight)), None

        init_state = (jnp.zeros((ROWS_DEV, D), jnp.float32), jnp.zeros((), jnp.float32))
        final_state, step_out = lax.scan(col_step, init_state, (blocks_x, blocks_q, blocks_sq, block_ids))
        return final_state

    forces, energies = lax.map(row_block, (blocks_x, blocks_q, blocks_sq, block_ids))
    return (forces / ELL_SQ).reshape(N_ROWS, D), (0.5 * jnp.sum(energies)).reshape(1)
```

```python
import math

import jax
import jax.numpy as jnp
from jax import lax
from jax.experimental import pallas as pl
from jax.experimental.pallas import tpu as pltpu
from jax.sharding import PartitionSpec as P

MESH = pl.DeviceIdType.MESH
TILE = 256
WIDE = 512
LANE = 128
GROUP = 16
LOG2E = math.log2(math.e)
F32 = jnp.float32
BF16 = jnp.bfloat16


def split3(val):
    high = val.astype(BF16).astype(F32)
    mid = (val - high).astype(BF16).astype(F32)
    return high, mid, val - high - mid


def kernel(n_row, x_hbm, q_ref, force_ref, energy_ref, left_op, pay, xit, aug, xt, qbc, pull, rsum, lim, sgn, sel, part, wbuf, ahead,
           load_sem, ring_send, ring_recv, pair_send, pair_recv, pay_send, pay_recv, ppair_send, ppair_recv, en_send, en_recv):
    n_blk, rows, _ = left_op.shape
    feat = x_hbm.shape[1]
    n_tile = rows // TILE
    n_wide = rows // WIDE
    n_chip = n_row // 2
    chunk = rows // 4
    scale = LOG2E / feat
    me = lax.axis_index("row")
    core = lax.rem(me, 2)
    chip = me // 2
    right = lax.rem(chip + 1, n_chip) * 2 + core
    left = lax.rem(chip + n_chip - 1, n_chip) * 2 + core
    pair = chip * 2 + (1 - core)
    x_lanes = pl.ds(0, feat)
    side_lanes = pl.ds(feat, LANE)

    load = pltpu.make_async_copy(x_hbm, left_op.at[0, :, x_lanes], load_sem)
    load.start()
    barrier = pltpu.get_barrier_semaphore()
    for k in range(1, n_row):
        pl.semaphore_signal(barrier, inc=1, device_id={"row": lax.rem(me + k, n_row)}, device_id_type=MESH)

    def remote(src, dst, send, recv, dev):
        return pltpu.make_async_remote_copy(src_ref=src, dst_ref=dst, send_sem=send, recv_sem=recv, device_id={"row": dev}, device_id_type=MESH)

    def part_of(u, pos):
        return left_op.at[u, pl.ds(pos * chunk, chunk), x_lanes]

    def ring(u, src_pos, to, pos):
        return remote(part_of(u, src_pos), part_of(to, pos), ring_send.at[to, pos], ring_recv.at[to, pos], right if pos == 0 else left)

    def to_pair(u):
        return remote(left_op.at[u, pl.ds(0, 2 * chunk), x_lanes], left_op.at[u, pl.ds(2 * chunk, 2 * chunk), x_lanes],
                      pair_send.at[u], pair_recv.at[u], pair)

    def pay_ring(src, step, pos):
        dst = 2 + step * 4 + pos
        return remote(pay.at[src], pay.at[dst], pay_send.at[step, pos], pay_recv.at[step, pos], right if pos == 0 else left)

    def pay_pair(step):
        at = 2 + step * 4
        return remote(pay.at[pl.ds(at, 2)], pay.at[pl.ds(at + 2, 2)], ppair_send.at[step + 1], ppair_recv.at[step + 1], pair)

    own_pair = remote(left_op.at[0, :, x_lanes], left_op.at[1, :, x_lanes], pair_send.at[1], pair_recv.at[1], pair)
    own_pay_pair = remote(pay.at[0], pay.at[1], ppair_send.at[0], ppair_recv.at[0], pair)

    load.wait()
    pl.semaphore_wait(barrier, n_row - 1)
    for pos in (0, 1):
        ring(0, 0, 2, pos).start()
    own_pair.start()

    lane = lax.broadcasted_iota(jnp.int32, (TILE, LANE), 1)
    table = jnp.zeros((TILE, LANE), F32)
    for g in range(n_tile):
        x32 = left_op[0, pl.ds(g * TILE, TILE), x_lanes].astype(F32)
        half = -0.5 * jnp.sum(x32 * x32, axis=1, keepdims=True)
        q_col = jnp.broadcast_to(q_ref[pl.ds(g, 1), :], (LANE, TILE)).T
        qbc[0, pl.ds(g * TILE, TILE), :] = q_col
        s_parts = split3(jnp.broadcast_to(half, (TILE, LANE)))
        q_parts = split3(q_col)
        base = g * GROUP
        for c, val in enumerate(s_parts + (jnp.ones((TILE, LANE), F32),)):
            hit = (lane >= base + c) & (lane < base + 6) if c == 3 else lane == base + c
            table = jnp.where(hit, val, table)
        for c, val in enumerate(q_parts):
            table = jnp.where(lane == base + 6 + c, val, table)
    pay[0] = table.astype(BF16)

    row_sel = lax.broadcasted_iota(jnp.int32, (LANE, TILE), 0)
    col_sel = lax.broadcasted_iota(jnp.int32, (LANE, TILE), 1) // LANE
    for k in range(n_tile // 2):
        at = row_sel - ((2 * k + col_sel) * GROUP + 6)
        sel[k] = jnp.where((at >= 0) & (at < 3), 1.0, 0.0).astype(BF16)

    own_pay_pair.start()
    for pos in (0, 1):
        pay_ring(0, 0, pos).start()
        for c in range(1, 4):
            ring(0, c, 2 + c, pos).start()

    def transposed(u, g):
        return left_op[u, pl.ds(g * TILE, TILE), x_lanes].T

    sub = lax.broadcasted_iota(jnp.int32, (GROUP, TILE), 0)
    for g in range(n_tile):
        t, cols = g * TILE // WIDE, pl.ds(g * TILE % WIDE, TILE)
        x_t = transposed(0, g)
        xit[t, :, cols] = x_t
        xt[0, :, pl.ds(g * TILE, TILE)] = x_t
        xt[1, :, pl.ds(g * TILE, TILE)] = jnp.zeros_like(x_t)
        left_op[0, pl.ds(g * TILE, TILE), side_lanes] = pay[0]
        x32 = x_t.astype(F32)
        q_row = q_ref[pl.ds(g, 1), :]
        q_log = feat * jnp.maximum(jnp.log(jnp.abs(q_row)), -200.0)
        lim[t, :, cols] = jnp.broadcast_to(q_log, (8, TILE))
        sgn[t, :, cols] = jnp.broadcast_to(jnp.where(q_row < 0.0, -1.0, 1.0), (8, TILE))
        shift = q_log - 0.5 * jnp.sum(x32 * x32, axis=0, keepdims=True)
        strip = jnp.where(sub < 3, 1.0, 0.0)
        for c, val in enumerate(split3(shift)):
            strip = jnp.where(sub == 3 + c, val, strip)
        strip = strip.astype(BF16)
        for k in range(n_tile):
            aug[k, t, :, cols] = jnp.zeros((LANE, TILE), BF16)
            aug[k, t, pl.ds(k * GROUP, GROUP), cols] = strip
    for t in range(n_wide):
        pull[t] = jnp.zeros((feat, WIDE), F32)
        rsum[t] = jnp.zeros((8, WIDE), F32)
    wbuf[...] = jnp.zeros_like(wbuf)

    def quarter_at(u, pos):
        return jnp.where(u < 2, pos, jnp.where(u >= n_blk - 2, u - (n_blk - 2) + 2 * (pos % 2), lax.rem(u + 2, 4)))

    def table_at(u, pos):
        return jnp.where(u < 2, u, ((u + 2) // 4) * 4 + pos - 2)

    def cross(u, t, g):
        rhs = jnp.concatenate([xit[t], aug[2 * quarter_at(u, g // 2) + g % 2, t]], axis=0)
        return jnp.dot(left_op[u, pl.ds(g * TILE, TILE), :], rhs, preferred_element_type=F32)

    def pulled(slot, t, g):
        at = pl.ds(g * TILE, TILE)
        pull[t] += jnp.dot(xt[slot, :, at], wbuf[at, :], preferred_element_type=F32)

    def prepare(u, slot, pos):
        strip = pay[table_at(u, pos)]
        wide = jnp.dot(strip, sel[quarter_at(u, pos)], preferred_element_type=F32)
        for h in (0, 1):
            at = pl.ds((2 * pos + h) * TILE, TILE)
            left_op[u, at, side_lanes] = strip
            qbc[slot, at, :] = wide[:, h * LANE:(h + 1) * LANE]
            xt[slot, :, at] = transposed(u, 2 * pos + h)

    def columns(u, t, own, todo):
        now = lax.rem(u, 2)
        nxt = jnp.minimum(u + 1, n_blk - 1)
        t_next = lax.rem(t + 1, n_wide)
        u_next = jnp.where(t == n_wide - 1, nxt, u)
        t_prev = lax.rem(t + n_wide - 1, n_wide)
        slot_prev = jnp.where(t == 0, 1 - now, now)
        bound = lim[t][None]
        sums = jnp.zeros((8, WIDE), F32)
        dots = ahead[...]
        for g in range(n_tile):
            pulled(slot_prev, t_prev, g)
            if g + 1 < n_tile:
                later = cross(u, t, g + 1)
            else:
                ahead[...] = cross(u_next, t_next, 0)
            if g % (n_tile // max(1, len(todo))) == 0 and todo:
                prepare(nxt, 1 - now, todo[g // (n_tile // len(todo))])
            at = pl.ds(g * TILE, TILE)
            q_col = qbc[now, at, :]
            kern = jnp.exp2(jnp.minimum(dots.reshape(TILE // 8, 8, WIDE), bound) * scale).reshape(TILE, WIDE)
            w = kern * jnp.concatenate([q_col] * (WIDE // LANE), axis=1)
            if own:
                r_id = lax.broadcasted_iota(jnp.int32, (TILE, WIDE), 0) + g * TILE
                c_id = lax.broadcasted_iota(jnp.int32, (TILE, WIDE), 1) + t * WIDE
                w = jnp.where(r_id == c_id, 0.0, w)
            sums = sums + jnp.sum(w.reshape(TILE // 8, 8, WIDE), axis=0)
            wbuf[at, :] = w.astype(BF16)
            if g + 1 < n_tile:
                dots = later
        rsum[t] += sums

    def pass_on(u):
        for pos in (0, 1):
            ring(u, pos, u, pos).wait_recv()
        to_pair(u).start()

        @pl.when(u < n_blk - 4)
        def _():
            ring(u, 0, u + 4, 0).start()

        @pl.when(u < n_blk - 6)
        def _():
            ring(u, 1, u + 4, 1).start()

        @pl.when((u >= n_blk - 4) & (u < n_blk - 2))
        def _():
            ring(u, 1, u + 2, 1).start()

        @pl.when(lax.rem(u, 4) == 2)
        def _():
            step = (u - 2) // 4
            for pos in (0, 1):
                pay_ring(2 + step * 4 + pos, step, pos).wait_recv()
            pay_pair(step).start()

            @pl.when(step < 3)
            def _():
                for pos in (0, 1):
                    pay_ring(2 + step * 4 + pos, step + 1, pos).start()

    half = n_wide // 2

    def loop(first, last, fn):
        def step(t, carry):
            fn(t)
            return carry

        lax.fori_loop(first, last, step, 0)

    chunks = [tuple(range(4))[k * 4 // half:(k + 1) * 4 // half] for k in range(half)]
    ahead[...] = cross(0, 0, 0)
    loop(0, half, lambda t: columns(0, t, True, ()))
    own_pair.wait_recv()
    own_pay_pair.wait_recv()
    for k in range(half):
        columns(0, half + k, True, chunks[k])

    def other(u):
        @pl.when(u < n_blk - 1)
        def _():
            pass_on(u + 1)

        loop(0, half, lambda t: columns(u, t, False, ()))

        @pl.when(u < n_blk - 1)
        def _():
            to_pair(u + 1).wait_recv()

            @pl.when(lax.rem(u + 1, 4) == 2)
            def _():
                pay_pair((u - 1) // 4).wait_recv()

        for k in range(half):
            columns(u, half + k, False, chunks[k])

    loop(1, n_blk, other)
    for g in range(n_tile):
        pulled((n_blk - 1) % 2, n_wide - 1, g)

    total = jnp.zeros((8, WIDE), F32)
    for t in range(n_wide):
        total = total + rsum[t] * sgn[t]
    part[me] = sum(total[:, k * LANE:(k + 1) * LANE] for k in range(WIDE // LANE))

    def finish(t):
        sums = jnp.sum(rsum[t], axis=0, keepdims=True)
        force_t = (sums * xit[t].astype(F32) - pull[t]) * (sgn[t, pl.ds(0, 1), :] * (1.0 / feat))
        force_ref[pl.ds(pl.multiple_of(t * WIDE, WIDE), WIDE), :] = force_t.T

    finish(0)

    def en_copy(k):
        return remote(part.at[me], part.at[me], en_send.at[k - 1], en_recv.at[k - 1], lax.rem(me + k, n_row))

    for k in range(1, n_row):
        en_copy(k).start()
    loop(1, n_wide, finish)

    for pos in (0, 1):
        for to in range(2, n_blk):
            ring(0, 0, to, pos).wait_send()
        for step in range(4):
            pay_ring(0, step, pos).wait_send()
    own_pair.wait_send()
    own_pay_pair.wait_send()
    for u in range(2, n_blk):
        to_pair(u).wait_send()
    for step in range(4):
        pay_pair(step).wait_send()
    for k in range(1, n_row):
        source = lax.rem(me + n_row - k, n_row)
        remote(part.at[source], part.at[source], en_send.at[k - 1], en_recv.at[k - 1], me).wait_recv()
        en_copy(k).wait_send()
    energy = part[0]
    for r in range(1, n_row):
        energy = energy + part[r]
    energy_ref[...] = jnp.broadcast_to(0.5 * jnp.sum(jnp.sum(energy, axis=0, keepdims=True), axis=1, keepdims=True), (8, LANE))


def solution(mesh):
    n_row = mesh.shape["row"]

    def device_body(pos_loc, chg_loc):
        rows, feat = pos_loc.shape
        n_tile, n_wide = rows // TILE, rows // WIDE
        vmem = pl.BlockSpec(memory_space=pltpu.VMEM)
        dma = pltpu.SemaphoreType.DMA
        force, energy = pl.pallas_call(
            lambda *refs: kernel(n_row, *refs),
            out_shape=(jax.ShapeDtypeStruct((rows, feat), F32), jax.ShapeDtypeStruct((8, LANE), F32)),
            in_specs=[pl.BlockSpec(memory_space=pl.ANY), vmem],
            out_specs=(vmem, vmem),
            scratch_shapes=[
                pltpu.VMEM((n_row, rows, feat + LANE), BF16),
                pltpu.VMEM((n_row + 2, TILE, LANE), BF16),
                pltpu.VMEM((n_wide, feat, WIDE), BF16),
                pltpu.VMEM((n_tile, n_wide, LANE, WIDE), BF16),
                pltpu.VMEM((2, feat, rows), BF16),
                pltpu.VMEM((2, rows, LANE), F32),
                pltpu.VMEM((n_wide, feat, WIDE), F32),
                pltpu.VMEM((n_wide, 8, WIDE), F32),
                pltpu.VMEM((n_wide, 8, WIDE), F32),
                pltpu.VMEM((n_wide, 8, WIDE), F32),
                pltpu.VMEM((n_tile // 2, LANE, TILE), BF16),
                pltpu.VMEM((n_row, 8, LANE), F32),
                pltpu.VMEM((rows, WIDE), BF16),
                pltpu.VMEM((TILE, WIDE), F32),
                dma,
                dma((n_row, 2)),
                dma((n_row, 2)),
                dma((n_row,)),
                dma((n_row,)),
                dma((4, 2)),
                dma((4, 2)),
                dma((5,)),
                dma((5,)),
                dma((n_row - 1,)),
                dma((n_row - 1,)),
            ],
            compiler_params=pltpu.CompilerParams(collective_id=0, has_side_effects=True, vmem_limit_bytes=60 * 2**20),
        )(pos_loc, chg_loc.reshape(n_tile, TILE))
        return force, energy[0, :1]

    return jax.shard_map(device_body, mesh=mesh, in_specs=(P(("sys", "row"), None), P(("sys", "row"))), out_specs=(P(("sys", "row"), None), P("sys")), check_vma=False)
```

```python
import math

import jax
import jax.numpy as jnp
from jax import lax
from jax.experimental import pallas as pl
from jax.experimental.pallas import tpu as pltpu
from jax.sharding import PartitionSpec as P

MESH = pl.DeviceIdType.MESH
TILE = 256
WIDE = 512
LANE = 128
GROUP = 16
LOG2E = math.log2(math.e)
F32 = jnp.float32
BF16 = jnp.bfloat16


def split3(val):
    high = val.astype(BF16).astype(F32)
    mid = (val - high).astype(BF16).astype(F32)
    return high, mid, val - high - mid


def kernel(n_row, x_hbm, q_ref, force_ref, energy_ref, xs, left_op, pay, xit, aug, xt, qbc, pull, rsum, lim, sgn, sel, part, mark, wbuf, ahead,
           load_sem, ring_send, ring_recv, pair_send, pair_recv, pay_send, pay_recv, ppair_send, ppair_recv, en_send, en_recv):
    n_blk, rows, feat = xs.shape
    n_tile = rows // TILE
    n_wide = rows // WIDE
    n_chip = n_row // 2
    chunk = rows // 4
    scale = LOG2E / feat
    me = lax.axis_index("row")
    core = lax.rem(me, 2)
    chip = me // 2
    right = lax.rem(chip + 1, n_chip) * 2 + core
    left = lax.rem(chip + n_chip - 1, n_chip) * 2 + core
    pair = chip * 2 + (1 - core)

    load = pltpu.make_async_copy(x_hbm, xs.at[0], load_sem)
    load.start()
    barrier = pltpu.get_barrier_semaphore()
    for k in range(1, n_row):
        pl.semaphore_signal(barrier, inc=1, device_id={"row": lax.rem(me + k, n_row)}, device_id_type=MESH)

    def remote(src, dst, send, recv, dev):
        return pltpu.make_async_remote_copy(src_ref=src, dst_ref=dst, send_sem=send, recv_sem=recv, device_id={"row": dev}, device_id_type=MESH)

    def quarter_of(u, c):
        return xs.at[u, pl.ds(c * chunk, chunk), :]

    def ring(src, to, c, pos):
        return remote(quarter_of(src, c), quarter_of(to, c), ring_send.at[to, c], ring_recv.at[to, c], right if pos == 0 else left)

    def pair_round(u):
        at, c = pl.ds(4 * ((u + 2) // 4) - 2, 2), lax.rem(u + 2, 4)
        dst = pl.ds(4 * ((u + 2) // 4), 2)
        rows_at = pl.ds(c * chunk, chunk)
        return remote(xs.at[at, rows_at, :], xs.at[dst, rows_at, :], pair_send.at[u], pair_recv.at[u], pair)

    def pay_ring(src, to, pos):
        return remote(pay.at[src], pay.at[to], pay_send.at[to], pay_recv.at[to], right if pos == 0 else left)

    def pay_pair(step):
        at = 2 + step * 4
        return remote(pay.at[pl.ds(at, 2)], pay.at[pl.ds(at + 2, 2)], ppair_send.at[step], ppair_recv.at[step], pair)

    own_pair = remote(xs.at[0], xs.at[1], pair_send.at[0], pair_recv.at[0], pair)
    own_pay_pair = remote(pay.at[0], pay.at[1], ppair_send.at[3], ppair_recv.at[3], pair)
    far_pair = remote(xs.at[n_blk - 2], xs.at[n_blk - 1], pair_send.at[1], pair_recv.at[1], pair)
    far_pay_pair = remote(pay.at[n_blk - 2], pay.at[n_blk - 1], ppair_send.at[4], ppair_recv.at[4], pair)

    load.wait()

    lane = lax.broadcasted_iota(jnp.int32, (TILE, LANE), 1)
    table = jnp.zeros((TILE, LANE), F32)
    for g in range(n_tile):
        x32 = xs[0, pl.ds(g * TILE, TILE), :].astype(F32)
        half = -0.5 * jnp.sum(x32 * x32, axis=1, keepdims=True)
        q_col = jnp.broadcast_to(q_ref[pl.ds(g * TILE, TILE)].reshape(1, TILE), (LANE, TILE)).T
        qbc[0, pl.ds(g * TILE, TILE), :] = q_col
        s_parts = split3(jnp.broadcast_to(half, (TILE, LANE)))
        q_parts = split3(q_col)
        base = g * GROUP
        for c, val in enumerate(s_parts + (jnp.ones((TILE, LANE), F32),)):
            hit = (lane >= base + c) & (lane < base + 6) if c == 3 else lane == base + c
            table = jnp.where(hit, val, table)
        for c, val in enumerate(q_parts):
            table = jnp.where(lane == base + 6 + c, val, table)
    pay[0] = table.astype(BF16)

    row_sel = lax.broadcasted_iota(jnp.int32, (LANE, TILE), 0)
    col_sel = lax.broadcasted_iota(jnp.int32, (LANE, TILE), 1) // LANE
    for k in range(n_tile // 2):
        at = row_sel - ((2 * k + col_sel) * GROUP + 6)
        sel[k] = jnp.where((at >= 0) & (at < 3), 1.0, 0.0).astype(BF16)

    pl.semaphore_wait(barrier, n_row - 1)
    for pos in (0, 1):
        ring(0, 2 + pos, 0, pos).start()
    own_pair.start()
    own_pay_pair.start()
    for pos in (0, 1):
        pay_ring(0, 2 + pos, pos).start()
        for c in range(1, 4):
            ring(0, 2 + pos, c, pos).start()

    def side_by_side(x, strip):
        return jnp.concatenate([x, strip], axis=1)

    sub = lax.broadcasted_iota(jnp.int32, (GROUP, TILE), 0)
    for g in range(n_tile):
        t, cols = g * TILE // WIDE, pl.ds(g * TILE % WIDE, TILE)
        x_own = xs[0, pl.ds(g * TILE, TILE), :]
        x_t = x_own.T
        xit[t, :, cols] = x_t
        xt[0, :, pl.ds(g * TILE, TILE)] = x_t
        xt[1, :, pl.ds(g * TILE, TILE)] = jnp.zeros_like(x_t)
        left_op[0, pl.ds(g * TILE, TILE), :] = side_by_side(x_own, pay[0])
        x32 = x_t.astype(F32)
        q_row = q_ref[pl.ds(g * TILE, TILE)].reshape(1, TILE)
        q_log = feat * jnp.maximum(jnp.log(jnp.abs(q_row)), -200.0)
        lim[t, :, cols] = jnp.broadcast_to(q_log, (8, TILE))
        sgn[t, :, cols] = jnp.broadcast_to(jnp.where(q_row < 0.0, -1.0, 1.0), (8, TILE))
        shift = q_log - 0.5 * jnp.sum(x32 * x32, axis=0, keepdims=True)
        strip = jnp.where(sub < 3, 1.0, 0.0)
        for c, val in enumerate(split3(shift)):
            strip = jnp.where(sub == 3 + c, val, strip)
        strip = strip.astype(BF16)
        for k in range(n_tile):
            aug[k, t, :, cols] = jnp.zeros((LANE, TILE), BF16)
            aug[k, t, pl.ds(k * GROUP, GROUP), cols] = strip
    for t in range(n_wide):
        pull[t] = jnp.zeros((feat, WIDE), F32)
        rsum[t] = jnp.zeros((8, WIDE), F32)
    wbuf[...] = jnp.zeros_like(wbuf)

    def slot_at(v, pos):
        half = pos // 2
        late = jnp.where(v < 12, 10 + 2 * half, jnp.where(v < 14, 14 + half, 11 + 2 * half))
        return jnp.where(v < 2, v, jnp.where(v < 10, 4 * ((v + 2) // 4) + pos - 2, late))

    def quarter_at(v, pos):
        return jnp.where(v < 2, pos, jnp.where(v < 10, lax.rem(v + 2, 4), 2 * lax.rem(v, 2) + pos % 2))

    def cross(v, slot, t, g):
        rhs = jnp.concatenate([xit[t], aug[2 * quarter_at(v, g // 2) + g % 2, t]], axis=0)
        return jnp.dot(left_op[slot, pl.ds(g * TILE, TILE), :], rhs, preferred_element_type=F32)

    def pulled(slot, t, g):
        at = pl.ds(g * TILE, TILE)
        pull[t] += jnp.dot(xt[slot, :, at], wbuf[at, :], preferred_element_type=F32)

    def prepare(v, slot):
        for pos in range(4):
            src, quarter = slot_at(v, pos), quarter_at(v, pos)
            strip = pay[src]
            wide = jnp.dot(strip, sel[quarter], preferred_element_type=F32)
            for h in (0, 1):
                at = pl.ds((2 * pos + h) * TILE, TILE)
                x = xs[src, pl.ds(pl.multiple_of(quarter * chunk + h * TILE, TILE), TILE), :]
                left_op[slot, at, :] = side_by_side(x, strip)
                qbc[slot, at, :] = wide[:, h * LANE:(h + 1) * LANE]
                xt[slot, :, at] = x.T

    def columns(u, t, own):
        now = lax.rem(u, 2)
        nxt = jnp.minimum(u + 1, n_blk - 1)
        t_next = lax.rem(t + 1, n_wide)
        wrap = t == n_wide - 1
        u_next, slot_next = jnp.where(wrap, nxt, u), jnp.where(wrap, 1 - now, now)
        t_prev = lax.rem(t + n_wide - 1, n_wide)
        slot_prev = jnp.where(t == 0, 1 - now, now)
        bound = lim[t][None]
        sums = jnp.zeros((8, WIDE), F32)
        dots = ahead[...]
        for g in range(n_tile):
            pulled(slot_prev, t_prev, g)
            if g + 1 < n_tile:
                later = cross(u, now, t, g + 1)
            else:
                ahead[...] = cross(u_next, slot_next, t_next, 0)
            at = pl.ds(g * TILE, TILE)
            q_col = qbc[now, at, :]
            kern = jnp.exp2(jnp.minimum(dots.reshape(TILE // 8, 8, WIDE), bound) * scale).reshape(TILE, WIDE)
            w = kern * jnp.concatenate([q_col] * (WIDE // LANE), axis=1)
            if own and g * TILE // WIDE == t:
                r_id = lax.broadcasted_iota(jnp.int32, (TILE, WIDE), 0) + g * TILE % WIDE
                c_id = lax.broadcasted_iota(jnp.int32, (TILE, WIDE), 1)
                w = jnp.where(r_id == c_id, 0.0, w)
            sums = sums + jnp.sum(w.reshape(TILE // 8, 8, WIDE), axis=0)
            wbuf[at, :] = w.astype(BF16)
            if g + 1 < n_tile:
                dots = later
        rsum[t] += sums

    def ring_round(u):
        at, c = 4 * ((u + 2) // 4) - 2, lax.rem(u + 2, 4)
        for pos in (0, 1):
            ring(at + pos, at + pos, c, pos).wait_recv()
        pair_round(u).start()

        @pl.when(u < 10)
        def _():
            for pos in (0, 1):
                ring(at + pos, at + pos + 4, c, pos).start()

        @pl.when((u >= 10) & (u < 12))
        def _():
            ring(at, n_blk - 2, c, 0).start()

        @pl.when(u >= 12)
        def _():
            ring(at + 1, n_blk - 2, c, 1).start()

        @pl.when(c == 0)
        def _():
            for pos in (0, 1):
                pay_ring(at + pos, at + pos, pos).wait_recv()
            pay_pair((u - 2) // 4).start()

            @pl.when(u < 10)
            def _():
                for pos in (0, 1):
                    pay_ring(at + pos, at + pos + 4, pos).start()

            @pl.when(u >= 10)
            def _():
                pay_ring(at, n_blk - 2, 0).start()

    def pair_wait(u):
        pair_round(u).wait_recv()

        @pl.when(lax.rem(u + 2, 4) == 0)
        def _():
            pay_pair((u - 2) // 4).wait_recv()

    def total():
        val = jnp.zeros((8, WIDE), F32)
        for t in range(n_wide):
            val = val + rsum[t] * sgn[t]
        return sum(val[:, k * LANE:(k + 1) * LANE] for k in range(WIDE // LANE))

    def en_copy(k):
        return remote(part.at[me], part.at[me], en_send.at[k - 1], en_recv.at[k - 1], lax.rem(me + k, n_row))

    def at_start(v):
        @pl.when(v < 9)
        def _():
            ring_round(v + 1)

        @pl.when(v == 9)
        def _():
            ring_round(v + 1)
            ring_round(v + 2)

        @pl.when(v == 10)
        def _():
            ring_round(v + 3)
            mark[0] = total()

        @pl.when(v == 11)
        def _():
            for c in range(4):
                ring(n_blk - 2, n_blk - 2, c, 0).wait_recv()
            pay_ring(n_blk - 2, n_blk - 2, 0).wait_recv()
            far_pair.start()
            far_pay_pair.start()

        @pl.when(v == 12)
        def _():
            mark[0] = total() - mark[0]

        @pl.when(v == 14)
        def _():
            part[me] = total() + mark[0]

    def at_middle(v):
        @pl.when(v < 9)
        def _():
            pair_wait(v + 1)

        @pl.when(v == 9)
        def _():
            pair_wait(v + 1)
            pair_wait(v + 2)
            ring_round(v + 3)

        @pl.when(v == 10)
        def _():
            pair_wait(v + 2)
            pair_wait(v + 3)

        @pl.when(v == 11)
        def _():
            far_pair.wait_recv()
            far_pay_pair.wait_recv()

        @pl.when(v == 14)
        def _():
            for k in range(1, n_row):
                en_copy(k).start()

    half = n_wide // 2

    def loop(first, last, fn):
        def step(t, carry):
            fn(t)
            return carry

        lax.fori_loop(first, last, step, 0)

    ahead[...] = cross(0, 0, 0, 0)
    for t in range(half):
        columns(0, t, True)
    own_pair.wait_recv()
    own_pay_pair.wait_recv()
    prepare(1, 1)
    for t in range(half, n_wide):
        columns(0, t, True)

    def other(v):
        at_start(v)
        loop(0, half, lambda t: columns(v, t, False))
        at_middle(v)
        prepare(jnp.minimum(v + 1, n_blk - 1), 1 - lax.rem(v, 2))
        loop(half, n_wide, lambda t: columns(v, t, False))

    loop(1, n_blk, other)
    for g in range(n_tile):
        pulled((n_blk - 1) % 2, n_wide - 1, g)

    def finish(t):
        sums = jnp.sum(rsum[t], axis=0, keepdims=True)
        force_t = (sums * xit[t].astype(F32) - pull[t]) * (sgn[t, pl.ds(0, 1), :] * (1.0 / feat))
        force_ref[pl.ds(pl.multiple_of(t * WIDE, WIDE), WIDE), :] = force_t.T

    loop(0, n_wide, finish)

    for to in range(2, n_blk - 1):
        if to < 14 and to % 4 > 1 or to == n_blk - 2:
            for c in range(4):
                ring(0, to, c, 0).wait_send()
            pay_ring(0, to, 0).wait_send()
    own_pair.wait_send()
    own_pay_pair.wait_send()
    far_pair.wait_send()
    far_pay_pair.wait_send()
    for u in range(2, 14):
        pair_round(u).wait_send()
    for step in range(3):
        pay_pair(step).wait_send()
    for k in range(1, n_row):
        source = lax.rem(me + n_row - k, n_row)
        remote(part.at[source], part.at[source], en_send.at[k - 1], en_recv.at[k - 1], me).wait_recv()
        en_copy(k).wait_send()
    energy = part[0]
    for r in range(1, n_row):
        energy = energy + part[r]
    energy_ref[...] = jnp.broadcast_to(0.5 * jnp.sum(jnp.sum(energy, axis=0, keepdims=True), axis=1, keepdims=True), (8, LANE))


def solution(mesh):
    n_row = mesh.shape["row"]

    def device_body(pos_loc, chg_loc):
        rows, feat = pos_loc.shape
        n_tile, n_wide = rows // TILE, rows // WIDE
        vmem = pl.BlockSpec(memory_space=pltpu.VMEM)
        dma = pltpu.SemaphoreType.DMA
        force, energy = pl.pallas_call(
            lambda *refs: kernel(n_row, *refs),
            out_shape=(jax.ShapeDtypeStruct((rows, feat), F32), jax.ShapeDtypeStruct((8, LANE), F32)),
            in_specs=[pl.BlockSpec(memory_space=pl.ANY), vmem],
            out_specs=(vmem, vmem),
            scratch_shapes=[
                pltpu.VMEM((n_row, rows, feat), BF16),
                pltpu.VMEM((2, rows, feat + LANE), BF16),
                pltpu.VMEM((n_row, TILE, LANE), BF16),
                pltpu.VMEM((n_wide, feat, WIDE), BF16),
                pltpu.VMEM((n_tile, n_wide, LANE, WIDE), BF16),
                pltpu.VMEM((2, feat, rows), BF16),
                pltpu.VMEM((2, rows, LANE), F32),
                pltpu.VMEM((n_wide, feat, WIDE), F32),
                pltpu.VMEM((n_wide, 8, WIDE), F32),
                pltpu.VMEM((n_wide, 8, WIDE), F32),
                pltpu.VMEM((n_wide, 8, WIDE), F32),
                pltpu.VMEM((n_tile // 2, LANE, TILE), BF16),
                pltpu.VMEM((n_row, 8, LANE), F32),
                pltpu.VMEM((1, 8, LANE), F32),
                pltpu.VMEM((rows, WIDE), BF16),
                pltpu.VMEM((TILE, WIDE), F32),
                dma,
                dma((n_row, 4)),
                dma((n_row, 4)),
                dma((n_row,)),
                dma((n_row,)),
                dma((n_row,)),
                dma((n_row,)),
                dma((5,)),
                dma((5,)),
                dma((n_row - 1,)),
                dma((n_row - 1,)),
            ],
            compiler_params=pltpu.CompilerParams(collective_id=0, has_side_effects=True, vmem_limit_bytes=36 * 2**20),
        )(pos_loc, chg_loc)
        return force, energy[0, :1]

    return jax.shard_map(device_body, mesh=mesh, in_specs=(P(("sys", "row"), None), P(("sys", "row"))), out_specs=(P(("sys", "row"), None), P("sys")), check_vma=False)
```

```python
import math

import jax
import jax.numpy as jnp
from jax import lax
from jax.experimental import pallas as pl
from jax.experimental.pallas import tpu as pltpu
from jax.sharding import PartitionSpec as P

MESH = pl.DeviceIdType.MESH
TILE = 256
WIDE = 512
LANE = 128
GROUP = 16
LOG2E = math.log2(math.e)
F32 = jnp.float32
BF16 = jnp.bfloat16


def split3(val):
    high = val.astype(BF16).astype(F32)
    mid = (val - high).astype(BF16).astype(F32)
    return high, mid, val - high - mid


def kernel(n_row, x_hbm, q_hbm, force_ref, energy_ref, q_ref, xs, left_op, pay, xit, aug, xt, qbc, pull, rsum, lim, sgn, sel, part, mark, wbuf, ahead,
           load_sem, load_q_sem, ring_send, ring_recv, pair_send, pair_recv, pay_send, pay_recv, ppair_send, ppair_recv, en_send, en_recv):
    n_blk, rows, feat = xs.shape
    n_tile = rows // TILE
    n_wide = rows // WIDE
    n_chip = n_row // 2
    chunk = rows // 4
    scale = LOG2E / feat
    me = lax.axis_index("row")
    core = lax.rem(me, 2)
    chip = me // 2
    right = lax.rem(chip + 1, n_chip) * 2 + core
    left = lax.rem(chip + n_chip - 1, n_chip) * 2 + core
    pair = chip * 2 + (1 - core)

    load = pltpu.make_async_copy(x_hbm, xs.at[0], load_sem)
    load.start()
    load_q = pltpu.make_async_copy(q_hbm, q_ref, load_q_sem)
    load_q.start()
    barrier = pltpu.get_barrier_semaphore()
    for k in range(1, n_row):
        pl.semaphore_signal(barrier, inc=1, device_id={"row": lax.rem(me + k, n_row)}, device_id_type=MESH)

    def loop(first, last, fn):
        def step(t, carry):
            fn(t)
            return carry

        lax.fori_loop(first, last, step, 0)

    def remote(src, dst, send, recv, dev):
        return pltpu.make_async_remote_copy(src_ref=src, dst_ref=dst, send_sem=send, recv_sem=recv, device_id={"row": dev}, device_id_type=MESH)

    def quarter_of(u, c):
        return xs.at[u, pl.ds(c * chunk, chunk), :]

    def ring(src, to, c, pos):
        return remote(quarter_of(src, c), quarter_of(to, c), ring_send.at[to, c], ring_recv.at[to, c], right if pos == 0 else left)

    def pair_round(u):
        at, c = pl.ds(4 * ((u + 2) // 4) - 2, 2), lax.rem(u + 2, 4)
        dst = pl.ds(4 * ((u + 2) // 4), 2)
        rows_at = pl.ds(c * chunk, chunk)
        return remote(xs.at[at, rows_at, :], xs.at[dst, rows_at, :], pair_send.at[u], pair_recv.at[u], pair)

    def pay_ring(src, to, pos):
        return remote(pay.at[src], pay.at[to], pay_send.at[to], pay_recv.at[to], right if pos == 0 else left)

    def pay_pair(step):
        at = 2 + step * 4
        return remote(pay.at[pl.ds(at, 2)], pay.at[pl.ds(at + 2, 2)], ppair_send.at[step], ppair_recv.at[step], pair)

    own_pair = remote(xs.at[0], xs.at[1], pair_send.at[0], pair_recv.at[0], pair)
    own_pay_pair = remote(pay.at[0], pay.at[1], ppair_send.at[3], ppair_recv.at[3], pair)
    far_pair = remote(xs.at[n_blk - 2], xs.at[n_blk - 1], pair_send.at[1], pair_recv.at[1], pair)
    far_pay_pair = remote(pay.at[n_blk - 2], pay.at[n_blk - 1], ppair_send.at[4], ppair_recv.at[4], pair)

    load.wait()
    load_q.wait()

    lane = lax.broadcasted_iota(jnp.int32, (TILE, LANE), 1)
    table = jnp.zeros((TILE, LANE), F32)
    for g in range(n_tile):
        x32 = xs[0, pl.ds(g * TILE, TILE), :].astype(F32)
        half = -0.5 * jnp.sum(x32 * x32, axis=1, keepdims=True)
        q_col = jnp.broadcast_to(q_ref[pl.ds(g * TILE, TILE)].reshape(1, TILE), (LANE, TILE)).T
        qbc[0, pl.ds(g * TILE, TILE), :] = q_col
        s_parts = split3(jnp.broadcast_to(half, (TILE, LANE)))
        q_parts = split3(q_col)
        base = g * GROUP
        for c, val in enumerate(s_parts + (jnp.ones((TILE, LANE), F32),)):
            hit = (lane >= base + c) & (lane < base + 6) if c == 3 else lane == base + c
            table = jnp.where(hit, val, table)
        for c, val in enumerate(q_parts):
            table = jnp.where(lane == base + 6 + c, val, table)
    pay[0] = table.astype(BF16)

    row_sel = lax.broadcasted_iota(jnp.int32, (LANE, TILE), 0)
    col_sel = lax.broadcasted_iota(jnp.int32, (LANE, TILE), 1) // LANE
    for k in range(n_tile // 2):
        at = row_sel - ((2 * k + col_sel) * GROUP + 6)
        sel[k] = jnp.where((at >= 0) & (at < 3), 1.0, 0.0).astype(BF16)

    pl.semaphore_wait(barrier, n_row - 1)
    for pos in (0, 1):
        ring(0, 2 + pos, 0, pos).start()
    own_pair.start()
    own_pay_pair.start()
    for pos in (0, 1):
        pay_ring(0, 2 + pos, pos).start()
        for c in range(1, 4):
            ring(0, 2 + pos, c, pos).start()

    def side_by_side(x, strip):
        return jnp.concatenate([x, strip], axis=1)

    sub = lax.broadcasted_iota(jnp.int32, (GROUP, TILE), 0)
    for g in range(n_tile):
        t, cols = g * TILE // WIDE, pl.ds(g * TILE % WIDE, TILE)
        x_own = xs[0, pl.ds(g * TILE, TILE), :]
        x_t = x_own.T
        xit[t, :, cols] = x_t
        xt[0, :, pl.ds(g * TILE, TILE)] = x_t
        left_op[0, pl.ds(g * TILE, TILE), :] = side_by_side(x_own, pay[0])
        x32 = x_t.astype(F32)
        q_row = q_ref[pl.ds(g * TILE, TILE)].reshape(1, TILE)
        q_log = feat * jnp.maximum(jnp.log(jnp.abs(q_row)), -200.0)
        lim[t, :, cols] = jnp.broadcast_to(q_log, (8, TILE))
        sgn[t, :, cols] = jnp.broadcast_to(jnp.where(q_row < 0.0, -1.0, 1.0), (8, TILE))
        shift = q_log - 0.5 * jnp.sum(x32 * x32, axis=0, keepdims=True)
        strip = jnp.where(sub < 3, 1.0, 0.0)
        for c, val in enumerate(split3(shift)):
            strip = jnp.where(sub == 3 + c, val, strip)
        strip = strip.astype(BF16)
        aug[t, :, cols] = jnp.zeros((2 * LANE - GROUP, TILE), BF16)
        aug[t, pl.ds(LANE - GROUP, GROUP), cols] = strip
    for t in range(n_wide):
        pull[t] = jnp.zeros((feat, WIDE), F32)
        rsum[t] = jnp.zeros((8, WIDE), F32)

    def slot_at(v, pos):
        half = pos // 2
        late = jnp.where(v < 12, 10 + 2 * half, jnp.where(v < 14, 14 + half, 11 + 2 * half))
        return jnp.where(v < 2, v, jnp.where(v < 10, 4 * ((v + 2) // 4) + pos - 2, late))

    def quarter_at(v, pos):
        return jnp.where(v < 2, pos, jnp.where(v < 10, lax.rem(v + 2, 4), 2 * lax.rem(v, 2) + pos % 2))

    def cross(v, slot, t, g):
        at = pl.multiple_of((n_tile - 1 - g % 2 - 2 * quarter_at(v, g // 2)) * GROUP, GROUP)
        rhs = jnp.concatenate([xit[t], aug[t, pl.ds(at, LANE), :]], axis=0)
        return jnp.dot(left_op[slot, pl.ds(g * TILE, TILE), :], rhs, preferred_element_type=F32)

    def pulled(slot, t, g):
        at = pl.ds(g * TILE, TILE)
        pull[t] += jnp.dot(xt[slot, :, at], wbuf[at, :], preferred_element_type=F32)

    def prepare(v, slot):
        for pos in range(4):
            src, quarter = slot_at(v, pos), quarter_at(v, pos)
            strip = pay[src]
            wide = jnp.dot(strip, sel[quarter], preferred_element_type=F32)
            for h in (0, 1):
                at = pl.ds((2 * pos + h) * TILE, TILE)
                x = xs[src, pl.ds(pl.multiple_of(quarter * chunk + h * TILE, TILE), TILE), :]
                left_op[slot, at, :] = side_by_side(x, strip)
                qbc[slot, at, :] = wide[:, h * LANE:(h + 1) * LANE]
                xt[slot, :, at] = x.T

    def columns(u, t, own):
        now = lax.rem(u, 2)
        nxt = jnp.minimum(u + 1, n_blk - 1)
        t_next = lax.rem(t + 1, n_wide)
        wrap = t == n_wide - 1
        u_next, slot_next = jnp.where(wrap, nxt, u), jnp.where(wrap, 1 - now, now)
        t_prev = lax.rem(t + n_wide - 1, n_wide)
        slot_prev = jnp.where(t == 0, 1 - now, now)
        bound = lim[t][None]
        sums = jnp.zeros((8, WIDE), F32)
        dots = ahead[...]
        for g in range(n_tile):
            if not (own and isinstance(t, int) and t == 0):
                pulled(slot_prev, t_prev, g)
            if g + 1 < n_tile:
                later = cross(u, now, t, g + 1)
            else:
                ahead[...] = cross(u_next, slot_next, t_next, 0)
            at = pl.ds(g * TILE, TILE)
            q_col = qbc[now, at, :]
            kern = jnp.exp2(jnp.minimum(dots.reshape(TILE // 8, 8, WIDE), bound) * scale).reshape(TILE, WIDE)
            w = kern * jnp.concatenate([q_col] * (WIDE // LANE), axis=1)
            if own and g * TILE // WIDE == t:
                r_id = lax.broadcasted_iota(jnp.int32, (TILE, WIDE), 0) + g * TILE % WIDE
                c_id = lax.broadcasted_iota(jnp.int32, (TILE, WIDE), 1)
                w = jnp.where(r_id == c_id, 0.0, w)
            sums = sums + jnp.sum(w.reshape(TILE // 8, 8, WIDE), axis=0)
            wbuf[at, :] = w.astype(BF16)
            if g + 1 < n_tile:
                dots = later
        rsum[t] += sums

    def ring_round(u):
        at, c = 4 * ((u + 2) // 4) - 2, lax.rem(u + 2, 4)
        for pos in (0, 1):
            ring(at + pos, at + pos, c, pos).wait_recv()
        pair_round(u).start()

        @pl.when(u < 10)
        def _():
            for pos in (0, 1):
                ring(at + pos, at + pos + 4, c, pos).start()

        @pl.when((u >= 10) & (u < 12))
        def _():
            ring(at, n_blk - 2, c, 0).start()

        @pl.when(u >= 12)
        def _():
            ring(at + 1, n_blk - 2, c, 1).start()

        @pl.when(c == 0)
        def _():
            for pos in (0, 1):
                pay_ring(at + pos, at + pos, pos).wait_recv()
            pay_pair((u - 2) // 4).start()

            @pl.when(u < 10)
            def _():
                for pos in (0, 1):
                    pay_ring(at + pos, at + pos + 4, pos).start()

            @pl.when(u >= 10)
            def _():
                pay_ring(at, n_blk - 2, 0).start()

    def pair_wait(u):
        pair_round(u).wait_recv()

        @pl.when(lax.rem(u + 2, 4) == 0)
        def _():
            pay_pair((u - 2) // 4).wait_recv()

    def total():
        val = jnp.zeros((8, WIDE), F32)
        for t in range(n_wide):
            val = val + rsum[t] * sgn[t]
        return sum(val[:, k * LANE:(k + 1) * LANE] for k in range(WIDE // LANE))

    def en_copy(k):
        return remote(part.at[me], part.at[me], en_send.at[k - 1], en_recv.at[k - 1], lax.rem(me + k, n_row))

    def at_start(v):
        @pl.when(v < 9)
        def _():
            ring_round(v + 1)

        @pl.when(v == 9)
        def _():
            ring_round(v + 1)
            ring_round(v + 2)

        @pl.when(v == 10)
        def _():
            ring_round(v + 3)
            mark[0] = total()

        @pl.when(v == 11)
        def _():
            for c in range(4):
                ring(n_blk - 2, n_blk - 2, c, 0).wait_recv()
            pay_ring(n_blk - 2, n_blk - 2, 0).wait_recv()
            far_pair.start()
            far_pay_pair.start()

        @pl.when(v == 12)
        def _():
            mark[0] = total() - mark[0]

        @pl.when(v == 14)
        def _():
            part[me] = total() + mark[0]

    def at_middle(v):
        @pl.when(v < 9)
        def _():
            pair_wait(v + 1)

        @pl.when(v == 9)
        def _():
            pair_wait(v + 1)
            pair_wait(v + 2)
            ring_round(v + 3)

        @pl.when(v == 10)
        def _():
            pair_wait(v + 2)
            pair_wait(v + 3)

        @pl.when(v == 11)
        def _():
            far_pair.wait_recv()
            far_pay_pair.wait_recv()

        @pl.when(v == 14)
        def _():
            loop(1, n_row, lambda k: en_copy(k).start())

    half = n_wide // 2

    ahead[...] = cross(0, 0, 0, 0)
    for t in range(half):
        columns(0, t, True)
    own_pair.wait_recv()
    own_pay_pair.wait_recv()
    prepare(1, 1)
    for t in range(half, n_wide):
        columns(0, t, True)

    def other(v):
        at_start(v)
        loop(0, half, lambda t: columns(v, t, False))
        at_middle(v)
        prepare(jnp.minimum(v + 1, n_blk - 1), 1 - lax.rem(v, 2))
        loop(half, n_wide, lambda t: columns(v, t, False))

    loop(1, n_blk, other)
    for g in range(n_tile):
        pulled((n_blk - 1) % 2, n_wide - 1, g)

    def finish(t):
        sums = jnp.sum(rsum[t], axis=0, keepdims=True)
        force_t = (sums * xit[t].astype(F32) - pull[t]) * (sgn[t, pl.ds(0, 1), :] * (1.0 / feat))
        force_ref[pl.ds(pl.multiple_of(t * WIDE, WIDE), WIDE), :] = force_t.T

    loop(0, n_wide, finish)

    for to in range(2, n_blk - 1):
        if to < 14 and to % 4 > 1 or to == n_blk - 2:
            for c in range(4):
                ring(0, to, c, 0).wait_send()
            pay_ring(0, to, 0).wait_send()
    own_pair.wait_send()
    own_pay_pair.wait_send()
    far_pair.wait_send()
    far_pay_pair.wait_send()
    for u in range(2, 14):
        pair_round(u).wait_send()
    for step in range(3):
        pay_pair(step).wait_send()
    for k in range(1, n_row):
        source = lax.rem(me + n_row - k, n_row)
        remote(part.at[source], part.at[source], en_send.at[k - 1], en_recv.at[k - 1], me).wait_recv()
        en_copy(k).wait_send()
    energy = part[0]
    for r in range(1, n_row):
        energy = energy + part[r]
    energy_ref[0] = 0.5 * jnp.sum(energy)


def solution(mesh):
    n_row = mesh.shape["row"]

    def device_body(pos_loc, chg_loc):
        rows, feat = pos_loc.shape
        n_tile, n_wide = rows // TILE, rows // WIDE
        vmem = pl.BlockSpec(memory_space=pltpu.VMEM)
        dma = pltpu.SemaphoreType.DMA
        return pl.pallas_call(
            lambda *refs: kernel(n_row, *refs),
            out_shape=(jax.ShapeDtypeStruct((rows, feat), F32), jax.ShapeDtypeStruct((1,), F32)),
            in_specs=[pl.BlockSpec(memory_space=pltpu.HBM)] * 2,
            out_specs=(vmem, pl.BlockSpec(memory_space=pltpu.SMEM)),
            scratch_shapes=[
                pltpu.VMEM((rows,), F32),
                pltpu.VMEM((n_row, rows, feat), BF16),
                pltpu.VMEM((2, rows, feat + LANE), BF16),
                pltpu.VMEM((n_row, TILE, LANE), BF16),
                pltpu.VMEM((n_wide, feat, WIDE), BF16),
                pltpu.VMEM((n_wide, 2 * LANE - GROUP, WIDE), BF16),
                pltpu.VMEM((2, feat, rows), BF16),
                pltpu.VMEM((2, rows, LANE), F32),
                pltpu.VMEM((n_wide, feat, WIDE), F32),
                pltpu.VMEM((n_wide, 8, WIDE), F32),
                pltpu.VMEM((n_wide, 8, WIDE), F32),
                pltpu.VMEM((n_wide, 8, WIDE), F32),
                pltpu.VMEM((n_tile // 2, LANE, TILE), BF16),
                pltpu.VMEM((n_row, 8, LANE), F32),
                pltpu.VMEM((1, 8, LANE), F32),
                pltpu.VMEM((rows, WIDE), BF16),
                pltpu.VMEM((TILE, WIDE), F32),
                dma,
                dma,
                dma((n_row, 4)),
                dma((n_row, 4)),
                dma((n_row,)),
                dma((n_row,)),
                dma((n_row,)),
                dma((n_row,)),
                dma((5,)),
                dma((5,)),
                dma((n_row - 1,)),
                dma((n_row - 1,)),
            ],
            compiler_params=pltpu.CompilerParams(collective_id=0, has_side_effects=True, vmem_limit_bytes=36 * 2**20),
        )(*(pltpu.with_memory_space_constraint(arg, pltpu.HBM) for arg in (pos_loc, chg_loc)))

    return jax.shard_map(device_body, mesh=mesh, in_specs=(P(("sys", "row"), None), P(("sys", "row"))), out_specs=(P(("sys", "row"), None), P("sys")), check_vma=False)
```

```python
import math

import jax
import jax.numpy as jnp
from jax import lax
from jax.experimental import pallas as pl
from jax.experimental.pallas import tpu as pltpu
from jax.sharding import PartitionSpec as P

MESH = pl.DeviceIdType.MESH
TILE = 256
WIDE = 512
LANE = 128
GROUP = 16
LOG2E = math.log2(math.e)
F32 = jnp.float32
BF16 = jnp.bfloat16


def split3(val):
    high = val.astype(BF16).astype(F32)
    mid = (val - high).astype(BF16).astype(F32)
    return high, mid, val - high - mid


def kernel(n_row, x_hbm, q_hbm, force_ref, energy_ref, q_ref, xs, left_op, pay, xit, aug, xt, qbc, pull, rsum, lim, sgn, sel, part, mark, wbuf, ahead,
           load_sem, load_q_sem, ring_send, ring_recv, pair_send, pair_recv, pay_send, pay_recv, ppair_send, ppair_recv, en_send, en_recv):
    n_blk, rows, feat = xs.shape
    n_tile = rows // TILE
    n_wide = rows // WIDE
    n_chip = n_row // 2
    chunk = rows // 4
    scale = LOG2E / feat
    me = lax.axis_index("row")
    core = lax.rem(me, 2)
    chip = me // 2
    right = lax.rem(chip + 1, n_chip) * 2 + core
    left = lax.rem(chip + n_chip - 1, n_chip) * 2 + core
    pair = chip * 2 + (1 - core)

    load = pltpu.make_async_copy(x_hbm, xs.at[0], load_sem)
    load.start()
    load_q = pltpu.make_async_copy(q_hbm, q_ref, load_q_sem)
    load_q.start()
    barrier = pltpu.get_barrier_semaphore()
    for k in range(1, n_row):
        pl.semaphore_signal(barrier, inc=1, device_id={"row": lax.rem(me + k, n_row)}, device_id_type=MESH)

    def loop(first, last, fn):
        def step(t, carry):
            fn(t)
            return carry

        lax.fori_loop(first, last, step, 0)

    def remote(src, dst, send, recv, dev):
        return pltpu.make_async_remote_copy(src_ref=src, dst_ref=dst, send_sem=send, recv_sem=recv, device_id={"row": dev}, device_id_type=MESH)

    def quarter_of(u, c):
        return xs.at[u, pl.ds(c * chunk, chunk), :]

    def ring(src, to, c, pos):
        return remote(quarter_of(src, c), quarter_of(to, c), ring_send.at[to, c], ring_recv.at[to, c], right if pos == 0 else left)

    def pair_round(u):
        at, c = pl.ds(4 * ((u + 2) // 4) - 2, 2), lax.rem(u + 2, 4)
        dst = pl.ds(4 * ((u + 2) // 4), 2)
        rows_at = pl.ds(c * chunk, chunk)
        return remote(xs.at[at, rows_at, :], xs.at[dst, rows_at, :], pair_send.at[u], pair_recv.at[u], pair)

    def pay_ring(src, to, pos):
        return remote(pay.at[src], pay.at[to], pay_send.at[to], pay_recv.at[to], right if pos == 0 else left)

    def pay_pair(step):
        at = 2 + step * 4
        return remote(pay.at[pl.ds(at, 2)], pay.at[pl.ds(at + 2, 2)], ppair_send.at[step], ppair_recv.at[step], pair)

    own_pair = remote(xs.at[0], xs.at[1], pair_send.at[0], pair_recv.at[0], pair)
    own_pay_pair = remote(pay.at[0], pay.at[1], ppair_send.at[3], ppair_recv.at[3], pair)
    far_pair = remote(xs.at[n_blk - 2], xs.at[n_blk - 1], pair_send.at[1], pair_recv.at[1], pair)
    far_pay_pair = remote(pay.at[n_blk - 2], pay.at[n_blk - 1], ppair_send.at[4], ppair_recv.at[4], pair)

    load.wait()
    load_q.wait()

    lane = lax.broadcasted_iota(jnp.int32, (TILE, LANE), 1)
    table = jnp.zeros((TILE, LANE), F32)
    for g in range(n_tile):
        x32 = xs[0, pl.ds(g * TILE, TILE), :].astype(F32)
        half = -0.5 * jnp.sum(x32 * x32, axis=1, keepdims=True)
        q_col = jnp.broadcast_to(q_ref[pl.ds(g * TILE, TILE)].reshape(1, TILE), (LANE, TILE)).T
        qbc[0, pl.ds(g * TILE, TILE), :] = q_col
        s_parts = split3(jnp.broadcast_to(half, (TILE, LANE)))
        q_parts = split3(q_col)
        base = g * GROUP
        for c, val in enumerate(s_parts + (jnp.ones((TILE, LANE), F32),)):
            hit = (lane >= base + c) & (lane < base + 6) if c == 3 else lane == base + c
            table = jnp.where(hit, val, table)
        for c, val in enumerate(q_parts):
            table = jnp.where(lane == base + 6 + c, val, table)
    pay[0] = table.astype(BF16)

    row_sel = lax.broadcasted_iota(jnp.int32, (LANE, TILE), 0)
    col_sel = lax.broadcasted_iota(jnp.int32, (LANE, TILE), 1) // LANE
    for k in range(n_tile // 2):
        at = row_sel - ((2 * k + col_sel) * GROUP + 6)
        sel[k] = jnp.where((at >= 0) & (at < 3), 1.0, 0.0).astype(BF16)

    pl.semaphore_wait(barrier, n_row - 1)
    for pos in (0, 1):
        ring(0, 2 + pos, 0, pos).start()
    own_pair.start()
    own_pay_pair.start()
    for pos in (0, 1):
        pay_ring(0, 2 + pos, pos).start()
        for c in range(1, 4):
            ring(0, 2 + pos, c, pos).start()

    def side_by_side(x, strip):
        return jnp.concatenate([x, strip], axis=1)

    sub = lax.broadcasted_iota(jnp.int32, (GROUP, TILE), 0)
    for g in range(n_tile):
        t, cols = g * TILE // WIDE, pl.ds(g * TILE % WIDE, TILE)
        x_own = xs[0, pl.ds(g * TILE, TILE), :]
        x_t = x_own.T
        xit[t, :, cols] = x_t
        xt[0, :, pl.ds(g * TILE, TILE)] = x_t
        left_op[0, pl.ds(g * TILE, TILE), :] = side_by_side(x_own, pay[0])
        x32 = x_t.astype(F32)
        q_row = q_ref[pl.ds(g * TILE, TILE)].reshape(1, TILE)
        q_log = feat * jnp.maximum(jnp.log(jnp.abs(q_row)), -200.0)
        lim[t, :, cols] = jnp.broadcast_to(q_log, (8, TILE))
        sgn[t, :, cols] = jnp.broadcast_to(jnp.where(q_row < 0.0, -1.0, 1.0), (8, TILE))
        shift = q_log - 0.5 * jnp.sum(x32 * x32, axis=0, keepdims=True)
        strip = jnp.where(sub < 3, 1.0, 0.0)
        for c, val in enumerate(split3(shift)):
            strip = jnp.where(sub == 3 + c, val, strip)
        strip = strip.astype(BF16)
        aug[t, :, cols] = jnp.zeros((2 * LANE - GROUP, TILE), BF16)
        aug[t, pl.ds(LANE - GROUP, GROUP), cols] = strip
    for t in range(n_wide):
        pull[t] = jnp.zeros((feat, WIDE), F32)
        rsum[t] = jnp.zeros((8, WIDE), F32)

    def slot_at(v, pos):
        half = pos // 2
        late = jnp.where(v < 12, 10 + 2 * half, jnp.where(v < 14, 14 + half, 11 + 2 * half))
        return jnp.where(v < 2, v, jnp.where(v < 10, 4 * ((v + 2) // 4) + pos - 2, late))

    def quarter_at(v, pos):
        return jnp.where(v < 2, pos, jnp.where(v < 10, lax.rem(v + 2, 4), 2 * lax.rem(v, 2) + pos % 2))

    def cross(v, slot, t, g):
        at = pl.multiple_of((n_tile - 1 - g % 2 - 2 * quarter_at(v, g // 2)) * GROUP, GROUP)
        rhs = jnp.concatenate([xit[t], aug[t, pl.ds(at, LANE), :]], axis=0)
        return jnp.dot(left_op[slot, pl.ds(g * TILE, TILE), :], rhs, preferred_element_type=F32)

    def pulled(slot, t, g):
        at = pl.ds(g * TILE, TILE)
        pull[t] += jnp.dot(xt[slot, :, at], wbuf[at, :], preferred_element_type=F32)

    def prepare(v, slot):
        for pos in range(4):
            src, quarter = slot_at(v, pos), quarter_at(v, pos)
            strip = pay[src]
            wide = jnp.dot(strip, sel[quarter], preferred_element_type=F32)
            for h in (0, 1):
                at = pl.ds((2 * pos + h) * TILE, TILE)
                x = xs[src, pl.ds(pl.multiple_of(quarter * chunk + h * TILE, TILE), TILE), :]
                left_op[slot, at, :] = side_by_side(x, strip)
                qbc[slot, at, :] = wide[:, h * LANE:(h + 1) * LANE]
                xt[slot, :, at] = x.T

    def columns(u, t, own):
        now = lax.rem(u, 2)
        nxt = jnp.minimum(u + 1, n_blk - 1)
        t_next = lax.rem(t + 1, n_wide)
        wrap = t == n_wide - 1
        u_next, slot_next = jnp.where(wrap, nxt, u), jnp.where(wrap, 1 - now, now)
        t_prev = lax.rem(t + n_wide - 1, n_wide)
        slot_prev = jnp.where(t == 0, 1 - now, now)
        bound = lim[t][None]
        sums = jnp.zeros((8, WIDE), F32)
        dots = ahead[...]
        for g in range(n_tile):
            if not (own and isinstance(t, int) and t == 0):
                pulled(slot_prev, t_prev, g)
            if g + 1 < n_tile:
                later = cross(u, now, t, g + 1)
            else:
                ahead[...] = cross(u_next, slot_next, t_next, 0)
            at = pl.ds(g * TILE, TILE)
            q_col = qbc[now, at, :]
            kern = jnp.exp2(jnp.minimum(dots.reshape(TILE // 8, 8, WIDE), bound) * scale).reshape(TILE, WIDE)
            w = kern * jnp.concatenate([q_col] * (WIDE // LANE), axis=1)
            if own and g * TILE // WIDE == t:
                r_id = lax.broadcasted_iota(jnp.int32, (TILE, WIDE), 0) + g * TILE % WIDE
                c_id = lax.broadcasted_iota(jnp.int32, (TILE, WIDE), 1)
                w = jnp.where(r_id == c_id, 0.0, w)
            sums = sums + jnp.sum(w.reshape(TILE // 8, 8, WIDE), axis=0)
            wbuf[at, :] = w.astype(BF16)
            if g + 1 < n_tile:
                dots = later
        rsum[t] += sums

    def ring_round(u):
        at, c = 4 * ((u + 2) // 4) - 2, lax.rem(u + 2, 4)
        for pos in (0, 1):
            ring(at + pos, at + pos, c, pos).wait_recv()
        pair_round(u).start()

        @pl.when(u < 10)
        def _():
            for pos in (0, 1):
                ring(at + pos, at + pos + 4, c, pos).start()

        @pl.when((u >= 10) & (u < 12))
        def _():
            ring(at, n_blk - 2, c, 0).start()

        @pl.when(u >= 12)
        def _():
            ring(at + 1, n_blk - 2, c, 1).start()

        @pl.when(c == 0)
        def _():
            for pos in (0, 1):
                pay_ring(at + pos, at + pos, pos).wait_recv()
            pay_pair((u - 2) // 4).start()

            @pl.when(u < 10)
            def _():
                for pos in (0, 1):
                    pay_ring(at + pos, at + pos + 4, pos).start()

            @pl.when(u >= 10)
            def _():
                pay_ring(at, n_blk - 2, 0).start()

    def pair_wait(u):
        pair_round(u).wait_recv()

        @pl.when(lax.rem(u + 2, 4) == 0)
        def _():
            pay_pair((u - 2) // 4).wait_recv()

    def total():
        val = jnp.zeros((8, WIDE), F32)
        for t in range(n_wide):
            val = val + rsum[t] * sgn[t]
        return sum(val[:, k * LANE:(k + 1) * LANE] for k in range(WIDE // LANE))

    def en_copy(k):
        return remote(part.at[me], part.at[me], en_send.at[k - 1], en_recv.at[k - 1], lax.rem(me + k, n_row))

    def at_start(v):
        @pl.when((v == 1) | (v == 3) | ((v >= 5) & (v <= 9)))
        def _():
            ring_round(jnp.where(v == 1, 2, jnp.where(v == 3, 5, jnp.where(v == 9, 12, v + 2))))

        @pl.when(v == 10)
        def _():
            mark[0] = total()

        @pl.when(v == 12)
        def _():
            mark[0] = total() - mark[0]

        @pl.when(v == 14)
        def _():
            part[me] = total() + mark[0]

    def at_middle(v):
        @pl.when(v < 9)
        def _():
            pair_wait(v + 1)

        @pl.when((v == 9) | (v == 10))
        def _():
            pair_wait(2 * v - 8)
            pair_wait(2 * v - 7)

        @pl.when(v == 11)
        def _():
            far_pair.wait_recv()
            far_pay_pair.wait_recv()

        @pl.when((v == 1) | (v == 2) | (v == 4) | (v == 8) | (v == 9))
        def _():
            ring_round(jnp.where(v == 8, 11, jnp.where(v == 9, 13, v + 2)))

        @pl.when(v == 10)
        def _():
            for c in range(4):
                ring(n_blk - 2, n_blk - 2, c, 0).wait_recv()
            pay_ring(n_blk - 2, n_blk - 2, 0).wait_recv()
            far_pair.start()
            far_pay_pair.start()

        @pl.when(v == 14)
        def _():
            loop(1, n_row, lambda k: en_copy(k).start())

    half = n_wide // 2

    ahead[...] = cross(0, 0, 0, 0)
    for t in range(half):
        columns(0, t, True)
    own_pair.wait_recv()
    own_pay_pair.wait_recv()
    prepare(1, 1)
    for t in range(half, n_wide):
        columns(0, t, True)

    def other(v):
        at_start(v)
        loop(0, half, lambda t: columns(v, t, False))
        at_middle(v)
        prepare(jnp.minimum(v + 1, n_blk - 1), 1 - lax.rem(v, 2))
        loop(half, n_wide, lambda t: columns(v, t, False))

    loop(1, n_blk, other)
    for g in range(n_tile):
        pulled((n_blk - 1) % 2, n_wide - 1, g)

    def finish(t):
        sums = jnp.sum(rsum[t], axis=0, keepdims=True)
        force_t = (sums * xit[t].astype(F32) - pull[t]) * (sgn[t, pl.ds(0, 1), :] * (1.0 / feat))
        force_ref[pl.ds(pl.multiple_of(t * WIDE, WIDE), WIDE), :] = force_t.T

    loop(0, n_wide, finish)

    for to in range(2, n_blk - 1):
        if to < 14 and to % 4 > 1 or to == n_blk - 2:
            for c in range(4):
                ring(0, to, c, 0).wait_send()
            pay_ring(0, to, 0).wait_send()
    own_pair.wait_send()
    own_pay_pair.wait_send()
    far_pair.wait_send()
    far_pay_pair.wait_send()
    for u in range(2, 14):
        pair_round(u).wait_send()
    for step in range(3):
        pay_pair(step).wait_send()
    for k in range(1, n_row):
        source = lax.rem(me + n_row - k, n_row)
        remote(part.at[source], part.at[source], en_send.at[k - 1], en_recv.at[k - 1], me).wait_recv()
        en_copy(k).wait_send()
    energy = part[0]
    for r in range(1, n_row):
        energy = energy + part[r]
    energy_ref[0] = 0.5 * jnp.sum(energy)


def solution(mesh):
    n_row = mesh.shape["row"]

    def device_body(pos_loc, chg_loc):
        rows, feat = pos_loc.shape
        n_tile, n_wide = rows // TILE, rows // WIDE
        vmem = pl.BlockSpec(memory_space=pltpu.VMEM)
        dma = pltpu.SemaphoreType.DMA
        return pl.pallas_call(
            lambda *refs: kernel(n_row, *refs),
            out_shape=(jax.ShapeDtypeStruct((rows, feat), F32), jax.ShapeDtypeStruct((1,), F32)),
            in_specs=[pl.BlockSpec(memory_space=pltpu.HBM)] * 2,
            out_specs=(vmem, pl.BlockSpec(memory_space=pltpu.SMEM)),
            scratch_shapes=[
                pltpu.VMEM((rows,), F32),
                pltpu.VMEM((n_row, rows, feat), BF16),
                pltpu.VMEM((2, rows, feat + LANE), BF16),
                pltpu.VMEM((n_row, TILE, LANE), BF16),
                pltpu.VMEM((n_wide, feat, WIDE), BF16),
                pltpu.VMEM((n_wide, 2 * LANE - GROUP, WIDE), BF16),
                pltpu.VMEM((2, feat, rows), BF16),
                pltpu.VMEM((2, rows, LANE), F32),
                pltpu.VMEM((n_wide, feat, WIDE), F32),
                pltpu.VMEM((n_wide, 8, WIDE), F32),
                pltpu.VMEM((n_wide, 8, WIDE), F32),
                pltpu.VMEM((n_wide, 8, WIDE), F32),
                pltpu.VMEM((n_tile // 2, LANE, TILE), BF16),
                pltpu.VMEM((n_row, 8, LANE), F32),
                pltpu.VMEM((1, 8, LANE), F32),
                pltpu.VMEM((rows, WIDE), BF16),
                pltpu.VMEM((TILE, WIDE), F32),
                dma,
                dma,
                dma((n_row, 4)),
                dma((n_row, 4)),
                dma((n_row,)),
                dma((n_row,)),
                dma((n_row,)),
                dma((n_row,)),
                dma((5,)),
                dma((5,)),
                dma((n_row - 1,)),
                dma((n_row - 1,)),
            ],
            compiler_params=pltpu.CompilerParams(collective_id=0, has_side_effects=True, vmem_limit_bytes=36 * 2**20),
        )(*(pltpu.with_memory_space_constraint(arg, pltpu.HBM) for arg in (pos_loc, chg_loc)))

    return jax.shard_map(device_body, mesh=mesh, in_specs=(P(("sys", "row"), None), P(("sys", "row"))), out_specs=(P(("sys", "row"), None), P("sys")), check_vma=False)
```

```python
import math

import jax
import jax.numpy as jnp
from jax import lax
from jax.experimental import pallas as pl
from jax.experimental.pallas import tpu as pltpu
from jax.sharding import PartitionSpec as P

MESH = pl.DeviceIdType.MESH
TILE = 256
WIDE = 512
LANE = 128
GROUP = 16
LOG2E = math.log2(math.e)
F32 = jnp.float32
BF16 = jnp.bfloat16


def split3(val):
    high = val.astype(BF16).astype(F32)
    mid = (val - high).astype(BF16).astype(F32)
    return high, mid, val - high - mid


def kernel(n_row, x_hbm, q_hbm, force_ref, energy_ref, q_ref, xs, left_op, pay, xit, aug, xt, qbc, pull, rsum, lim, sgn, sel, part, mark, wbuf, ahead,
           load_sem, load_q_sem, ring_send, ring_recv, pair_send, pair_recv, pay_send, pay_recv, ppair_send, ppair_recv, en_send, en_recv):
    n_blk, rows, feat = xs.shape
    n_tile = rows // TILE
    n_wide = rows // WIDE
    n_chip = n_row // 2
    chunk = rows // 4
    scale = LOG2E / feat
    me = lax.axis_index("row")
    core = lax.rem(me, 2)
    chip = me // 2
    right = lax.rem(chip + 1, n_chip) * 2 + core
    left = lax.rem(chip + n_chip - 1, n_chip) * 2 + core
    pair = chip * 2 + (1 - core)

    load = pltpu.make_async_copy(x_hbm, xs.at[0], load_sem)
    load.start()
    load_q = pltpu.make_async_copy(q_hbm, q_ref, load_q_sem)
    load_q.start()
    barrier = pltpu.get_barrier_semaphore()
    for k in range(1, n_row):
        pl.semaphore_signal(barrier, inc=1, device_id={"row": lax.rem(me + k, n_row)}, device_id_type=MESH)

    def loop(first, last, fn):
        def step(t, carry):
            fn(t)
            return carry

        lax.fori_loop(first, last, step, 0)

    def remote(src, dst, send, recv, dev):
        return pltpu.make_async_remote_copy(src_ref=src, dst_ref=dst, send_sem=send, recv_sem=recv, device_id={"row": dev}, device_id_type=MESH)

    def quarter_of(u, c):
        return xs.at[u, pl.ds(c * chunk, chunk), :]

    def ring(src, to, c, pos):
        return remote(quarter_of(src, c), quarter_of(to, c), ring_send.at[to, c], ring_recv.at[to, c], right if pos == 0 else left)

    def pair_round(u):
        at, c = pl.ds(4 * ((u + 2) // 4) - 2, 2), lax.rem(u + 2, 4)
        dst = pl.ds(4 * ((u + 2) // 4), 2)
        rows_at = pl.ds(c * chunk, chunk)
        return remote(xs.at[at, rows_at, :], xs.at[dst, rows_at, :], pair_send.at[u], pair_recv.at[u], pair)

    def pay_ring(src, to, pos):
        return remote(pay.at[src], pay.at[to], pay_send.at[to], pay_recv.at[to], right if pos == 0 else left)

    def pay_pair(step):
        at = 2 + step * 4
        return remote(pay.at[pl.ds(at, 2)], pay.at[pl.ds(at + 2, 2)], ppair_send.at[step], ppair_recv.at[step], pair)

    own_pair = remote(xs.at[0], xs.at[1], pair_send.at[0], pair_recv.at[0], pair)
    own_pay_pair = remote(pay.at[0], pay.at[1], ppair_send.at[3], ppair_recv.at[3], pair)
    far_pair = remote(xs.at[n_blk - 2], xs.at[n_blk - 1], pair_send.at[1], pair_recv.at[1], pair)
    far_pay_pair = remote(pay.at[n_blk - 2], pay.at[n_blk - 1], ppair_send.at[4], ppair_recv.at[4], pair)

    load.wait()
    load_q.wait()

    lane = lax.broadcasted_iota(jnp.int32, (TILE, LANE), 1)
    table = jnp.zeros((TILE, LANE), F32)
    for g in range(n_tile):
        x32 = xs[0, pl.ds(g * TILE, TILE), :].astype(F32)
        half = -0.5 * jnp.sum(x32 * x32, axis=1, keepdims=True)
        q_col = jnp.broadcast_to(q_ref[pl.ds(g * TILE, TILE)].reshape(1, TILE), (LANE, TILE)).T
        qbc[0, pl.ds(g * TILE, TILE), :] = q_col
        s_parts = split3(jnp.broadcast_to(half, (TILE, LANE)))
        q_parts = split3(q_col)
        base = g * GROUP
        for c, val in enumerate(s_parts + (jnp.ones((TILE, LANE), F32),)):
            hit = (lane >= base + c) & (lane < base + 6) if c == 3 else lane == base + c
            table = jnp.where(hit, val, table)
        for c, val in enumerate(q_parts):
            table = jnp.where(lane == base + 6 + c, val, table)
    pay[0] = table.astype(BF16)

    row_sel = lax.broadcasted_iota(jnp.int32, (LANE, TILE), 0)
    col_sel = lax.broadcasted_iota(jnp.int32, (LANE, TILE), 1) // LANE
    for k in range(n_tile // 2):
        at = row_sel - ((2 * k + col_sel) * GROUP + 6)
        sel[k] = jnp.where((at >= 0) & (at < 3), 1.0, 0.0).astype(BF16)

    pl.semaphore_wait(barrier, n_row - 1)
    for pos in (0, 1):
        ring(0, 2 + pos, 0, pos).start()
    own_pair.start()
    own_pay_pair.start()
    for pos in (0, 1):
        pay_ring(0, 2 + pos, pos).start()
        for c in range(1, 4):
            ring(0, 2 + pos, c, pos).start()

    def side_by_side(x, strip):
        return jnp.concatenate([x, strip], axis=1)

    sub = lax.broadcasted_iota(jnp.int32, (GROUP, TILE), 0)
    for g in range(n_tile):
        t, cols = g * TILE // WIDE, pl.ds(g * TILE % WIDE, TILE)
        x_own = xs[0, pl.ds(g * TILE, TILE), :]
        x_t = x_own.T
        xit[t, :, cols] = x_t
        xt[0, :, pl.ds(g * TILE, TILE)] = x_t
        left_op[0, pl.ds(g * TILE, TILE), :] = side_by_side(x_own, pay[0])
        x32 = x_t.astype(F32)
        q_row = q_ref[pl.ds(g * TILE, TILE)].reshape(1, TILE)
        q_log = feat * jnp.maximum(jnp.log(jnp.abs(q_row)), -200.0)
        lim[t, :, cols] = jnp.broadcast_to(q_log, (8, TILE))
        sgn[t, :, cols] = jnp.broadcast_to(jnp.where(q_row < 0.0, -1.0, 1.0), (8, TILE))
        shift = q_log - 0.5 * jnp.sum(x32 * x32, axis=0, keepdims=True)
        strip = jnp.where(sub < 3, 1.0, 0.0)
        for c, val in enumerate(split3(shift)):
            strip = jnp.where(sub == 3 + c, val, strip)
        strip = strip.astype(BF16)
        for k in range(n_tile):
            aug[k, t, :, cols] = jnp.zeros((LANE, TILE), BF16)
            aug[k, t, pl.ds(k * GROUP, GROUP), cols] = strip
    for t in range(n_wide):
        pull[t] = jnp.zeros((feat, WIDE), F32)
        rsum[t] = jnp.zeros((8, WIDE), F32)

    def slot_at(v, pos):
        half = pos // 2
        late = jnp.where(v < 12, 10 + 2 * half, jnp.where(v < 14, 14 + half, 11 + 2 * half))
        return jnp.where(v < 2, v, jnp.where(v < 10, 4 * ((v + 2) // 4) + pos - 2, late))

    def quarter_at(v, pos):
        return jnp.where(v < 2, pos, jnp.where(v < 10, lax.rem(v + 2, 4), 2 * lax.rem(v, 2) + pos % 2))

    def cross(v, slot, t, g):
        rhs = jnp.concatenate([xit[t], aug[2 * quarter_at(v, g // 2) + g % 2, t]], axis=0)
        return jnp.dot(left_op[slot, pl.ds(g * TILE, TILE), :], rhs, preferred_element_type=F32)

    def pulled(slot, t, g):
        at = pl.ds(g * TILE, TILE)
        pull[t] += jnp.dot(xt[slot, :, at], wbuf[at, :], preferred_element_type=F32)

    def prepare(v, slot):
        for pos in range(4):
            src, quarter = slot_at(v, pos), quarter_at(v, pos)
            strip = pay[src]
            wide = jnp.dot(strip, sel[quarter], preferred_element_type=F32)
            for h in (0, 1):
                at = pl.ds((2 * pos + h) * TILE, TILE)
                x = xs[src, pl.ds(pl.multiple_of(quarter * chunk + h * TILE, TILE), TILE), :]
                left_op[slot, at, :] = side_by_side(x, strip)
                qbc[slot, at, :] = wide[:, h * LANE:(h + 1) * LANE]
                xt[slot, :, at] = x.T

    def columns(u, t, own):
        now = lax.rem(u, 2)
        nxt = jnp.minimum(u + 1, n_blk - 1)
        t_next = lax.rem(t + 1, n_wide)
        wrap = t == n_wide - 1
        u_next, slot_next = jnp.where(wrap, nxt, u), jnp.where(wrap, 1 - now, now)
        t_prev = lax.rem(t + n_wide - 1, n_wide)
        slot_prev = jnp.where(t == 0, 1 - now, now)
        bound = lim[t][None]
        sums = jnp.zeros((8, WIDE), F32)
        dots = ahead[...]
        for g in range(n_tile):
            if not (own and isinstance(t, int) and t == 0):
                pulled(slot_prev, t_prev, g)
            if g + 1 < n_tile:
                later = cross(u, now, t, g + 1)
            else:
                ahead[...] = cross(u_next, slot_next, t_next, 0)
            at = pl.ds(g * TILE, TILE)
            q_col = qbc[now, at, :]
            kern = jnp.exp2(jnp.minimum(dots.reshape(TILE // 8, 8, WIDE), bound) * scale).reshape(TILE, WIDE)
            w = kern * jnp.concatenate([q_col] * (WIDE // LANE), axis=1)
            if own and g * TILE // WIDE == t:
                r_id = lax.broadcasted_iota(jnp.int32, (TILE, WIDE), 0) + g * TILE % WIDE
                c_id = lax.broadcasted_iota(jnp.int32, (TILE, WIDE), 1)
                w = jnp.where(r_id == c_id, 0.0, w)
            sums = sums + jnp.sum(w.reshape(TILE // 8, 8, WIDE), axis=0)
            wbuf[at, :] = w.astype(BF16)
            if g + 1 < n_tile:
                dots = later
        rsum[t] += sums

    def ring_round(u):
        at, c = 4 * ((u + 2) // 4) - 2, lax.rem(u + 2, 4)
        for pos in (0, 1):
            ring(at + pos, at + pos, c, pos).wait_recv()
        pair_round(u).start()

        @pl.when(u < 10)
        def _():
            for pos in (0, 1):
                ring(at + pos, at + pos + 4, c, pos).start()

        @pl.when((u >= 10) & (u < 12))
        def _():
            ring(at, n_blk - 2, c, 0).start()

        @pl.when(u >= 12)
        def _():
            ring(at + 1, n_blk - 2, c, 1).start()

        @pl.when(c == 0)
        def _():
            for pos in (0, 1):
                pay_ring(at + pos, at + pos, pos).wait_recv()
            pay_pair((u - 2) // 4).start()

            @pl.when(u < 10)
            def _():
                for pos in (0, 1):
                    pay_ring(at + pos, at + pos + 4, pos).start()

            @pl.when(u >= 10)
            def _():
                pay_ring(at, n_blk - 2, 0).start()

    def pair_wait(u):
        pair_round(u).wait_recv()

        @pl.when(lax.rem(u + 2, 4) == 0)
        def _():
            pay_pair((u - 2) // 4).wait_recv()

    def total():
        val = jnp.zeros((8, WIDE), F32)
        for t in range(n_wide):
            val = val + rsum[t] * sgn[t]
        return sum(val[:, k * LANE:(k + 1) * LANE] for k in range(WIDE // LANE))

    def en_copy(k):
        return remote(part.at[me], part.at[me], en_send.at[k - 1], en_recv.at[k - 1], lax.rem(me + k, n_row))

    def at_start(v):
        @pl.when((v == 1) | (v == 3) | ((v >= 5) & (v <= 9)))
        def _():
            ring_round(jnp.where(v == 1, 2, jnp.where(v == 3, 5, jnp.where(v == 9, 12, v + 2))))

        @pl.when(v == 10)
        def _():
            mark[0] = total()

        @pl.when(v == 12)
        def _():
            mark[0] = total() - mark[0]

        @pl.when(v == 14)
        def _():
            part[me] = total() + mark[0]

    def at_middle(v):
        @pl.when(v < 9)
        def _():
            pair_wait(v + 1)

        @pl.when((v == 9) | (v == 10))
        def _():
            pair_wait(2 * v - 8)
            pair_wait(2 * v - 7)

        @pl.when(v == 11)
        def _():
            far_pair.wait_recv()
            far_pay_pair.wait_recv()

        @pl.when((v == 1) | (v == 2) | (v == 4) | (v == 8) | (v == 9))
        def _():
            ring_round(jnp.where(v == 8, 11, jnp.where(v == 9, 13, v + 2)))

        @pl.when(v == 10)
        def _():
            for c in range(4):
                ring(n_blk - 2, n_blk - 2, c, 0).wait_recv()
            pay_ring(n_blk - 2, n_blk - 2, 0).wait_recv()
            far_pair.start()
            far_pay_pair.start()

        @pl.when(v == 14)
        def _():
            loop(1, n_row, lambda k: en_copy(k).start())

    half = n_wide // 2

    ahead[...] = cross(0, 0, 0, 0)
    for t in range(half):
        columns(0, t, True)
    own_pair.wait_recv()
    own_pay_pair.wait_recv()
    prepare(1, 1)
    for t in range(half, n_wide):
        columns(0, t, True)

    def other(v):
        at_start(v)
        loop(0, half, lambda t: columns(v, t, False))
        at_middle(v)
        prepare(jnp.minimum(v + 1, n_blk - 1), 1 - lax.rem(v, 2))
        loop(half, n_wide, lambda t: columns(v, t, False))

    loop(1, n_blk, other)
    for g in range(n_tile):
        pulled((n_blk - 1) % 2, n_wide - 1, g)

    def finish(t):
        sums = jnp.sum(rsum[t], axis=0, keepdims=True)
        force_t = (sums * xit[t].astype(F32) - pull[t]) * (sgn[t, pl.ds(0, 1), :] * (1.0 / feat))
        force_ref[pl.ds(pl.multiple_of(t * WIDE, WIDE), WIDE), :] = force_t.T

    loop(0, n_wide, finish)

    for to in range(2, n_blk - 1):
        if to < 14 and to % 4 > 1 or to == n_blk - 2:
            for c in range(4):
                ring(0, to, c, 0).wait_send()
            pay_ring(0, to, 0).wait_send()
    own_pair.wait_send()
    own_pay_pair.wait_send()
    far_pair.wait_send()
    far_pay_pair.wait_send()
    for u in range(2, 14):
        pair_round(u).wait_send()
    for step in range(3):
        pay_pair(step).wait_send()
    for k in range(1, n_row):
        source = lax.rem(me + n_row - k, n_row)
        remote(part.at[source], part.at[source], en_send.at[k - 1], en_recv.at[k - 1], me).wait_recv()
        en_copy(k).wait_send()
    energy = part[0]
    for r in range(1, n_row):
        energy = energy + part[r]
    energy_ref[0] = 0.5 * jnp.sum(energy)


def solution(mesh):
    n_row = mesh.shape["row"]

    def device_body(pos_loc, chg_loc):
        rows, feat = pos_loc.shape
        n_tile, n_wide = rows // TILE, rows // WIDE
        vmem = pl.BlockSpec(memory_space=pltpu.VMEM)
        dma = pltpu.SemaphoreType.DMA
        return pl.pallas_call(
            lambda *refs: kernel(n_row, *refs),
            out_shape=(jax.ShapeDtypeStruct((rows, feat), F32), jax.ShapeDtypeStruct((1,), F32)),
            in_specs=[pl.BlockSpec(memory_space=pltpu.HBM)] * 2,
            out_specs=(vmem, pl.BlockSpec(memory_space=pltpu.SMEM)),
            scratch_shapes=[
                pltpu.VMEM((rows,), F32),
                pltpu.VMEM((n_row, rows, feat), BF16),
                pltpu.VMEM((2, rows, feat + LANE), BF16),
                pltpu.VMEM((n_row, TILE, LANE), BF16),
                pltpu.VMEM((n_wide, feat, WIDE), BF16),
                pltpu.VMEM((n_tile, n_wide, LANE, WIDE), BF16),
                pltpu.VMEM((2, feat, rows), BF16),
                pltpu.VMEM((2, rows, LANE), F32),
                pltpu.VMEM((n_wide, feat, WIDE), F32),
                pltpu.VMEM((n_wide, 8, WIDE), F32),
                pltpu.VMEM((n_wide, 8, WIDE), F32),
                pltpu.VMEM((n_wide, 8, WIDE), F32),
                pltpu.VMEM((n_tile // 2, LANE, TILE), BF16),
                pltpu.VMEM((n_row, 8, LANE), F32),
                pltpu.VMEM((1, 8, LANE), F32),
                pltpu.VMEM((rows, WIDE), BF16),
                pltpu.VMEM((TILE, WIDE), F32),
                dma,
                dma,
                dma((n_row, 4)),
                dma((n_row, 4)),
                dma((n_row,)),
                dma((n_row,)),
                dma((n_row,)),
                dma((n_row,)),
                dma((5,)),
                dma((5,)),
                dma((n_row - 1,)),
                dma((n_row - 1,)),
            ],
            compiler_params=pltpu.CompilerParams(collective_id=0, has_side_effects=True, vmem_limit_bytes=36 * 2**20),
        )(*(pltpu.with_memory_space_constraint(arg, pltpu.HBM) for arg in (pos_loc, chg_loc)))

    return jax.shard_map(device_body, mesh=mesh, in_specs=(P(("sys", "row"), None), P(("sys", "row"))), out_specs=(P(("sys", "row"), None), P("sys")), check_vma=False)
```
